8 devices in a mesh: fields: 1 (over z), col: 2 (over y), row: 4 (over x, core).
Axes of the slice: x: 2, y: 2, z: 1, core: 2. Of those that a mesh axis runs over, the one named last changes fastest.
Arguments:
- field_u: bfloat16 [12, 256, 256, 256], P('fields', None, 'row', 'col')
- fac_a: bfloat16 [256, 256], P('fields')
- fac_b: bfloat16 [256, 256], P('fields')
- fac_c: bfloat16 [256, 256], P('fields')
- diag_d: float32 [256, 256, 256], P(('fields', 'row'), 'col')
Outputs:
- output: float32 [12, 256, 256, 256], P('fields', None, 'row', 'col')
All inputs are finite; a program needn't handle non-finite values.
Results may differ from the reference program's by a relative error of at most 0.00205687.
Values are sent between devices in bfloat16 or wider.
A program may use at most 1 GiB of HBM per device.

```python
import jax
import jax.numpy as jnp
from jax import lax

N = 256
BATCH = 12


def setup_inputs(seed: int = 0, part: int = 0) -> dict:
    base_key = jax.random.fold_in(jax.random.key(seed), part)
    key_field, key_a, key_b, key_c, key_diag = jax.random.split(base_key, 5)
    fan_scale = N ** -0.5
    field_u = jax.random.normal(key_field, (BATCH, N, N, N), jnp.float32)
    fac_a = jax.random.normal(key_a, (N, N), jnp.float32) * fan_scale
    fac_b = jax.random.normal(key_b, (N, N), jnp.float32) * fan_scale
    fac_c = jax.random.normal(key_c, (N, N), jnp.float32) * fan_scale
    diag_d = jnp.exp(0.5 * jax.random.normal(key_diag, (N, N, N), jnp.float32))
    return {"field_u": field_u.astype(jnp.bfloat16), "fac_a": fac_a.astype(jnp.bfloat16), "fac_b": fac_b.astype(jnp.bfloat16), "fac_c": fac_c.astype(jnp.bfloat16), "diag_d": diag_d}


def reference(field_u, fac_a, fac_b, fac_c, diag_d):
    mat_a = fac_a.astype(jnp.float32)
    mat_b = fac_b.astype(jnp.float32)
    mat_c = fac_c.astype(jnp.float32)
    scales = diag_d.astype(jnp.float32)

    def to_bf16(values_in):
        return values_in.astype(jnp.bfloat16).astype(jnp.float32)

    def one_tensor(tensor):
        stage_one = to_bf16(jnp.einsum("ix,xyz->iyz", mat_a, tensor.astype(jnp.float32)))
        stage_two = to_bf16(jnp.einsum("jy,iyz->ijz", mat_b, stage_one))
        stage_three = to_bf16(jnp.einsum("kz,ijz->ijk", mat_c, stage_two) * scales)
        stage_four = to_bf16(jnp.einsum("kz,ijk->ijz", mat_c, stage_three))
        stage_five = to_bf16(jnp.einsum("jy,ijz->iyz", mat_b, stage_four))
        return jnp.einsum("ix,iyz->xyz", mat_a, stage_five)

    return lax.map(one_tensor, field_u)
```

```python
import jax
import jax.numpy as jnp
from jax import lax
from jax.experimental import pallas as pl
from jax.experimental.pallas import tpu as pltpu
from jax.sharding import PartitionSpec as P


BF = jnp.bfloat16
F32 = jnp.float32

FIRST = (16, 16, 32)
MID = (32, 32)
LAST = (32, 16, 16)


def slabs(batch):
    return [FIRST] + [MID] * (batch - 2) + [LAST]


ORDER = (
    (1, 0, (0,)), (1, 0, (1,)), (1, 0, (2,)), (2, 0, 0), (2, 0, 1), (1, 1, (0, 1)), (3, 0, 0), (3, 0, 1),
    (2, 0, 2), (1, 2, (0, 1)), (2, 1, 0), (2, 1, 1), (5, 0, 0), (5, 0, 1), (3, 0, 2), (1, 3, (0, 1)),
    (3, 1, 0), (3, 1, 1), (1, 4, (0, 1)), (2, 2, 0), (2, 2, 1), (5, 0, 2), (2, 3, 0), (5, 1, 0), (2, 3, 1),
    (5, 1, 1), (2, 4, 0), (3, 2, 0), (1, 5, (0, 1)), (3, 2, 1), (2, 4, 1), (6, 0, 0), (3, 3, 0),
    (1, 6, (0, 1)), (3, 3, 1), (6, 1, 0), (3, 4, 0), (1, 7, (0, 1)), (5, 2, 0), (2, 5, 0), (5, 2, 1),
    (2, 5, 1), (2, 6, 0), (3, 4, 1), (2, 6, 1), (5, 3, 0), (2, 7, 0), (5, 3, 1), (2, 7, 1), (5, 4, 0),
    (3, 5, 0), (1, 8, (0, 1)), (3, 5, 1), (6, 2, 0), (3, 6, 0), (1, 9, (0, 1)), (5, 4, 1), (6, 3, 0),
    (3, 6, 1), (2, 8, 0), (3, 7, 0), (1, 10, (0, 1)), (3, 7, 1), (2, 8, 1), (2, 9, 0), (5, 5, 0), (2, 9, 1),
    (5, 5, 1), (6, 4, 0), (5, 6, 0), (2, 10, 0), (5, 6, 1), (2, 10, 1), (3, 8, 0), (1, 11, (0, 1, 2)),
    (5, 7, 0), (6, 5, 0), (5, 7, 1), (3, 8, 1), (6, 6, 0), (3, 9, 0), (2, 11, 0), (2, 11, 1), (3, 9, 1),
    (2, 11, 2), (3, 10, 0), (3, 10, 1), (6, 7, 0), (5, 8, 0), (5, 8, 1), (5, 9, 0), (6, 8, 0), (3, 11, 0),
    (3, 11, 1), (5, 9, 1), (3, 11, 2), (5, 10, 0), (6, 9, 0), (5, 10, 1), (5, 11, 0), (5, 11, 1), (6, 10, 0),
    (5, 11, 2), (6, 11, 0),
)


def dot(a, b):
    return jnp.dot(a, b, preferred_element_type=F32)


def any_spec():
    return pl.BlockSpec(memory_space=pl.ANY)


def whole(shape):
    return pl.BlockSpec(shape, lambda *g: (0,) * len(shape))


def call(body, token, ins, in_specs, outs, out_specs, grid, name, flops, alias=None):
    n_in, n_out = len(ins), len(outs)

    def wrapped(token_ref, *refs):
        body(refs[:n_in], refs[n_in:n_in + n_out])

    aliases = {0: n_out}
    aliases.update(alias or {})
    results = pl.pallas_call(
        wrapped,
        grid=grid,
        in_specs=[any_spec()] + list(in_specs),
        out_specs=list(out_specs) + [any_spec()],
        out_shape=list(outs) + [jax.ShapeDtypeStruct(token.shape, token.dtype)],
        input_output_aliases=aliases,
        cost_estimate=pl.CostEstimate(flops=flops, bytes_accessed=1 << 20, transcendentals=0),
        name=name,
    )(token, *ins)
    return results[:-1], results[-1]


def stage_one(token, u, a4, b, parts, ny, nz, yb=16):
    nx = u.shape[1]
    rows = 4 * sum(s for _, s in parts)

    def body(ins, outs):
        u_ref, a_ref = ins
        a = jnp.concatenate([a_ref[k, o:o + s, :] for o, s in parts for k in range(4)], axis=0)
        flat = u_ref[0].reshape(nx, yb * nz)
        h = dot(a, flat).astype(BF).reshape(rows, yb, nz)
        at = 0
        for n, (o, s) in enumerate(parts):
            for k in range(4):
                outs[4 * n + k][...] = h[at:at + s]
                at += s

    outs = [jax.ShapeDtypeStruct((s, ny, nz), BF) for _, s in parts for _ in range(4)]
    out_specs = [pl.BlockSpec((s, yb, nz), lambda g: (0, g, 0)) for _, s in parts for _ in range(4)]
    return call(body, token, (u, a4), [pl.BlockSpec((1, nx, yb, nz), lambda g: (b, 0, g, 0)), whole(a4.shape)],
                outs, out_specs, (ny // yb,), f"s1_{b}", 2 * rows * nx * ny * nz)


def stage_two(token, pieces, b4, name, ti=8):
    size, ny, nz = pieces[0].shape
    nj = b4.shape[0] // 2

    def body(ins, outs):
        bm = ins[4][...]
        for i in range(0, ti, 2):
            y = jnp.concatenate([jnp.concatenate([ins[k][i + e] for k in range(4)], axis=0) for e in range(2)], axis=1)
            h = dot(bm, y).astype(BF)
            for e in range(2):
                for l in range(2):
                    outs[l][i + e] = h[l * nj:(l + 1) * nj, e * nz:(e + 1) * nz]

    out = jax.ShapeDtypeStruct((size, nj, nz), BF)
    return call(body, token, (*pieces, b4), [pl.BlockSpec((ti, ny, nz), lambda g: (g, 0, 0))] * 4 + [whole(b4.shape)],
                [out] * 2, [pl.BlockSpec((ti, nj, nz), lambda g: (g, 0, 0))] * 2, (size // ti,), name,
                2 * size * 4 * ny * 2 * nj * nz)


def stage_three_four(token, own, got, c_in, c_out, diag, offset, name, ti=8):
    size, nj, nz = own.shape
    nk = c_out.shape[0]

    def body(ins, outs):
        own_ref, got_ref, ci_ref, co_ref, d_ref = ins
        ci, co = ci_ref[...], co_ref[...]
        for i in range(0, ti, 2):
            z = jnp.concatenate([jnp.concatenate([own_ref[i + e], got_ref[i + e]], axis=1) for e in range(2)], axis=0)
            h3 = (dot(z, ci) * d_ref[i:i + 2].reshape(2 * nj, nk)).astype(BF)
            h4 = dot(h3, co).astype(BF)
            for e in range(2):
                for l in range(2):
                    outs[l][i + e] = h4[e * nj:(e + 1) * nj, l * nz:(l + 1) * nz]

    first = offset // ti
    block = pl.BlockSpec((ti, nj, nz), lambda g: (g, 0, 0))
    out = jax.ShapeDtypeStruct((size, nj, nz), BF)
    return call(body, token, (own, got, c_in, c_out, diag),
                [block] * 2 + [whole(c_in.shape), whole(c_out.shape), pl.BlockSpec((ti, nj, nk), lambda g: (first + g, 0, 0))],
                [out] * 2, [block] * 2, (size // ti,), name, 4 * size * nj * 2 * nz * nk)


def stage_five(token, own, got, b5, name, ti=8):
    size, nj, nz = own.shape
    ny = b5.shape[0] // 4

    def body(ins, outs):
        bm = ins[2][...]
        for i in range(0, ti, 2):
            j = jnp.concatenate([jnp.concatenate([ins[l][i + e] for l in range(2)], axis=0) for e in range(2)], axis=1)
            h = dot(bm, j).astype(BF)
            for e in range(2):
                for k in range(4):
                    outs[k][i + e] = h[k * ny:(k + 1) * ny, e * nz:(e + 1) * nz]

    out = jax.ShapeDtypeStruct((size, ny, nz), BF)
    return call(body, token, (own, got, b5), [pl.BlockSpec((ti, nj, nz), lambda g: (g, 0, 0))] * 2 + [whole(b5.shape)],
                [out] * 4, [pl.BlockSpec((ti, ny, nz), lambda g: (g, 0, 0))] * 4, (size // ti,), name,
                2 * size * 2 * nj * 4 * ny * nz)


def stage_six(token, pieces, a6, w, b, batch, yb=16):
    nx = a6.shape[0]
    _, ny, nz = pieces[0].shape
    n = len(pieces)

    def body(ins, outs):
        x = jnp.concatenate([ref[...] for ref in ins[:n]], axis=0).reshape(a6.shape[1], yb * nz)
        outs[0][0] = dot(ins[n][...], x).reshape(nx, yb, nz)

    ins = (*pieces, a6)
    in_specs = [pl.BlockSpec((p.shape[0], yb, nz), lambda g: (0, g, 0)) for p in pieces] + [whole(a6.shape)]
    alias = None
    if w is not None:
        ins += (w,)
        in_specs.append(any_spec())
        alias = {len(ins): 0}
    (w,), token = call(body, token, ins, in_specs, [jax.ShapeDtypeStruct((batch, nx, ny, nz), F32)],
                       [pl.BlockSpec((1, nx, yb, nz), lambda g: (b, 0, g, 0))], (ny // yb,), f"s6_{b}",
                       2 * nx * nx * ny * nz, alias)
    return w, token


def solution(mesh):
    spec_field = P("fields", None, "row", "col")
    spec_factor = P("fields", None)
    spec_diag = P(("fields", "row"), "col", None)

    def over_row(value, k):
        return lax.ppermute(value, "row", [(r, r ^ k) for r in range(4)])

    def over_col(value):
        return lax.ppermute(value, "col", [(0, 1), (1, 0)])

    def local_apply(u, a, bm, cm, diag):
        batch, nx, ny, nz = u.shape
        r, c = lax.axis_index("row"), lax.axis_index("col")
        peers = jnp.bitwise_xor(r, jnp.arange(4))
        sides = jnp.bitwise_xor(c, jnp.arange(2))
        slab = nx // 4
        a4 = jnp.take(a.reshape(4, slab, nx), peers, axis=0)
        a6 = a4.reshape(nx, nx).T
        b4 = jnp.take(bm.reshape(2, nx // 2, 4, nx // 4), sides, axis=0)
        b4 = jnp.take(b4, peers, axis=2).reshape(nx, nx)
        b5 = b4.T
        c_out = jnp.take(cm.reshape(nx, 2, nx // 2), sides, axis=1).reshape(nx, nx)
        c_in = c_out.T
        token = jnp.zeros((8, 128), F32)
        cuts = slabs(batch)
        starts = [[sum(cut[:q]) for q in range(len(cut))] for cut in cuts]
        y_in, z_in, j_in, x_in = {}, {}, {}, {}
        w = None
        for kind, b, q in ORDER:
            if kind == 1:
                parts = [(starts[b][n], cuts[b][n]) for n in q]
                outs, token = stage_one(token, u, a4, b, parts, ny, nz)
                for n, part in enumerate(q):
                    o = outs[4 * n:4 * n + 4]
                    y_in[b, part] = [o[0]] + [over_row(o[k], k) for k in (1, 2, 3)]
            elif kind == 2:
                (own, other), token = stage_two(token, y_in.pop((b, q)), b4, f"s2_{b}_{q}")
                z_in[b, q] = (own, over_col(other))
            elif kind == 3:
                own, got = z_in.pop((b, q))
                (own, other), token = stage_three_four(token, own, got, c_in, c_out, diag, starts[b][q], f"s34_{b}_{q}")
                j_in[b, q] = (own, over_col(other))
            elif kind == 5:
                own, got = j_in.pop((b, q))
                o, token = stage_five(token, own, got, b5, f"s5_{b}_{q}")
                x_in[b, q] = [o[0]] + [over_row(o[k], k) for k in (1, 2, 3)]
            else:
                pieces = [x_in[b, n][k] for k in range(4) for n in range(len(cuts[b]))]
                w, token = stage_six(token, pieces, a6, w, b, batch)
        return w

    return jax.shard_map(local_apply, mesh=mesh, in_specs=(spec_field, spec_factor, spec_factor, spec_factor, spec_diag), out_specs=spec_field, check_vma=False)
```

```python
import jax
import jax.numpy as jnp
from jax import lax
from jax.experimental import pallas as pl
from jax.experimental.pallas import tpu as pltpu
from jax.sharding import PartitionSpec as P


BF = jnp.bfloat16
F32 = jnp.float32
UNROLL = 2

SLABS = (
    (8, 8, 16, 32,),
    (32, 32,),
    (64,),
    (64,),
    (64,),
    (64,),
    (64,),
    (64,),
    (64,),
    (64,),
    (32, 32,),
    (32, 16, 8, 8,),
)


ORDER = (
    (1, 0, (0, 1, 2, 3)), (2, 0, 1), (2, 0, 0), (3, 0, 1), (2, 0, 2), (3, 0, 0), (1, 1, (0, 1)), (3, 0, 2),
    (2, 0, 3), (1, 8, (0,)), (2, 1, 0), (2, 1, 1), (1, 4, (0,)), (1, 3, (0,)), (3, 0, 3), (1, 5, (0,)),
    (3, 1, 0), (2, 8, 0), (3, 1, 1), (2, 3, 0), (1, 6, (0,)), (2, 4, 0), (3, 8, 0), (1, 11, (0, 1, 2, 3)),
    (1, 10, (0, 1)), (3, 4, 0), (1, 9, (0,)), (2, 6, 0), (2, 5, 0), (1, 2, (0,)), (5, 4, 0), (2, 2, 0),
    (3, 5, 0), (5, 0, 1), (5, 1, 1), (1, 7, (0,)), (3, 3, 0), (3, 2, 0), (2, 7, 0), (5, 5, 0), (5, 3, 0),
    (5, 8, 0), (3, 6, 0), (3, 7, 0), (5, 2, 0), (6, 5, 0), (2, 9, 0), (6, 4, 0), (5, 1, 0), (5, 7, 0),
    (6, 2, 0), (5, 6, 0), (2, 10, 1), (2, 10, 0), (3, 9, 0), (6, 7, 0), (6, 1, 0), (5, 0, 3), (2, 11, 0),
    (3, 10, 1), (2, 11, 2), (5, 0, 0), (6, 3, 0), (3, 10, 0), (5, 0, 2), (6, 6, 0), (5, 9, 0), (3, 11, 0),
    (5, 10, 1), (2, 11, 3), (6, 0, 0), (2, 11, 1), (5, 10, 0), (6, 9, 0), (5, 11, 0), (3, 11, 2), (3, 11, 3),
    (6, 8, 0), (3, 11, 1), (5, 11, 2), (5, 11, 3), (5, 11, 1), (6, 10, 0), (6, 11, 0),
)


def dot(a, b):
    return jnp.dot(a, b, preferred_element_type=F32)


def any_spec():
    return pl.BlockSpec(memory_space=pl.ANY)


def whole(shape):
    return pl.BlockSpec(shape, lambda *g: (0,) * len(shape))


def call(body, token, ins, in_specs, outs, out_specs, grid, flops, alias=None):
    n_in, n_out = len(ins), len(outs)

    def wrapped(token_ref, *refs):
        body(refs[:n_in], refs[n_in:n_in + n_out])

    aliases = {0: n_out}
    aliases.update(alias or {})
    results = pl.pallas_call(
        wrapped,
        grid=grid,
        in_specs=[any_spec()] + list(in_specs),
        out_specs=list(out_specs) + [any_spec()],
        out_shape=list(outs) + [jax.ShapeDtypeStruct(token.shape, token.dtype)],
        input_output_aliases=aliases,
        cost_estimate=pl.CostEstimate(flops=flops, bytes_accessed=1 << 20, transcendentals=0),
        compiler_params=pltpu.CompilerParams(vmem_limit_bytes=67043328),
    )(token, *ins)
    return results[:-1], results[-1]


def stage_one(token, u, a4, b, parts, ny, nz, yb=16, sub=8):
    nx = u.shape[1]
    rows = 4 * sum(s for _, s in parts)

    def body(ins, outs):
        u_ref, a_ref = ins
        a = jnp.concatenate([a_ref[k, o:o + s, :] for o, s in parts for k in range(4)], axis=0)

        def step(t, carry):
            at_y = pl.ds(pl.multiple_of(t * sub, sub), sub)
            flat = u_ref[0, :, at_y, :].reshape(nx, sub * nz)
            h = dot(a, flat).astype(BF).reshape(rows, sub, nz)
            at = 0
            for n, (o, s) in enumerate(parts):
                for k in range(4):
                    outs[4 * n + k][:, at_y, :] = h[at:at + s]
                    at += s
            return carry

        lax.fori_loop(0, yb // sub, step, 0)

    outs = [jax.ShapeDtypeStruct((s, ny, nz), BF) for _, s in parts for _ in range(4)]
    out_specs = [pl.BlockSpec((s, yb, nz), lambda g: (0, g, 0)) for _, s in parts for _ in range(4)]
    return call(body, token, (u, a4), [pl.BlockSpec((1, nx, yb, nz), lambda g: (b, 0, g, 0)), whole(a4.shape)],
                outs, out_specs, (ny // yb,), 2 * rows * nx * ny * nz)


def stage_two(token, pieces, b4, ti=8):
    size, ny, nz = pieces[0].shape
    nj = b4.shape[0] // 2

    def body(ins, outs):
        bm = ins[4][...]

        def step(t, carry):
            i = 2 * t
            y = jnp.concatenate([jnp.concatenate([ins[k][i + e] for k in range(4)], axis=0) for e in range(2)], axis=1)
            h = dot(bm, y).astype(BF)
            for e in range(2):
                for l in range(2):
                    outs[l][i + e] = h[l * nj:(l + 1) * nj, e * nz:(e + 1) * nz]
            return carry

        lax.fori_loop(0, ti // 2, step, 0, unroll=UNROLL)

    out = jax.ShapeDtypeStruct((size, nj, nz), BF)
    return call(body, token, (*pieces, b4), [pl.BlockSpec((ti, ny, nz), lambda g: (g, 0, 0))] * 4 + [whole(b4.shape)],
                [out] * 2, [pl.BlockSpec((ti, nj, nz), lambda g: (g, 0, 0))] * 2, (size // ti,),
                2 * size * 4 * ny * 2 * nj * nz)


def stage_three_four(token, own, got, c_in, c_out, diag, offset, ti=8):
    size, nj, nz = own.shape
    nk = c_out.shape[0]

    def body(ins, outs):
        own_ref, got_ref, ci_ref, co_ref, d_ref = ins
        ci, co = ci_ref[...], co_ref[...]

        def step(t, carry):
            i = 2 * t
            z = jnp.concatenate([jnp.concatenate([own_ref[i + e], got_ref[i + e]], axis=1) for e in range(2)], axis=0)
            h3 = (dot(z, ci) * d_ref[pl.ds(i, 2)].reshape(2 * nj, nk)).astype(BF)
            h4 = dot(h3, co).astype(BF)
            for e in range(2):
                for l in range(2):
                    outs[l][i + e] = h4[e * nj:(e + 1) * nj, l * nz:(l + 1) * nz]
            return carry

        lax.fori_loop(0, ti // 2, step, 0, unroll=UNROLL)

    first = offset // ti
    block = pl.BlockSpec((ti, nj, nz), lambda g: (g, 0, 0))
    out = jax.ShapeDtypeStruct((size, nj, nz), BF)
    return call(body, token, (own, got, c_in, c_out, diag),
                [block] * 2 + [whole(c_in.shape), whole(c_out.shape), pl.BlockSpec((ti, nj, nk), lambda g: (first + g, 0, 0))],
                [out] * 2, [block] * 2, (size // ti,), 4 * size * nj * 2 * nz * nk)


def stage_five(token, own, got, b5, ti=8):
    size, nj, nz = own.shape
    ny = b5.shape[0] // 4

    def body(ins, outs):
        bm = ins[2][...]

        def step(t, carry):
            i = 2 * t
            j = jnp.concatenate([jnp.concatenate([ins[l][i + e] for l in range(2)], axis=0) for e in range(2)], axis=1)
            h = dot(bm, j).astype(BF)
            for e in range(2):
                for k in range(4):
                    outs[k][i + e] = h[k * ny:(k + 1) * ny, e * nz:(e + 1) * nz]
            return carry

        lax.fori_loop(0, ti // 2, step, 0, unroll=UNROLL)

    out = jax.ShapeDtypeStruct((size, ny, nz), BF)
    return call(body, token, (own, got, b5), [pl.BlockSpec((ti, nj, nz), lambda g: (g, 0, 0))] * 2 + [whole(b5.shape)],
                [out] * 4, [pl.BlockSpec((ti, ny, nz), lambda g: (g, 0, 0))] * 4, (size // ti,),
                2 * size * 2 * nj * 4 * ny * nz)


def stage_six(token, pieces, a6, w, b, batch, yb=16, sub=8):
    nx = a6.shape[0]
    _, ny, nz = pieces[0].shape
    n = len(pieces)

    def body(ins, outs):
        def step(t, carry):
            at_y = pl.ds(pl.multiple_of(t * sub, sub), sub)
            x = jnp.concatenate([ref[:, at_y, :] for ref in ins[:n]], axis=0).reshape(a6.shape[1], sub * nz)
            outs[0][0, :, at_y, :] = dot(ins[n][...], x).reshape(nx, sub, nz)
            return carry

        lax.fori_loop(0, yb // sub, step, 0)

    ins = (*pieces, a6)
    in_specs = [pl.BlockSpec((p.shape[0], yb, nz), lambda g: (0, g, 0)) for p in pieces] + [whole(a6.shape)]
    alias = None
    if w is not None:
        ins += (w,)
        in_specs.append(any_spec())
        alias = {len(ins): 0}
    (w,), token = call(body, token, ins, in_specs, [jax.ShapeDtypeStruct((batch, nx, ny, nz), F32)],
                       [pl.BlockSpec((1, nx, yb, nz), lambda g: (b, 0, g, 0))], (ny // yb,),
                       2 * nx * nx * ny * nz, alias)
    return w, token


def solution(mesh):
    spec_field = P("fields", None, "row", "col")
    spec_factor = P("fields", None)
    spec_diag = P(("fields", "row"), "col", None)

    def over_row(outs, m=0):
        got = {}
        for k in (2, 3, 1):
            got[k] = lax.ppermute(outs[k], "row", [(r, r ^ k) for r in range(4)])
            m += 1
        return [outs[0], got[1], got[2], got[3]]

    def over_col(value):
        return lax.ppermute(value, "col", [(0, 1), (1, 0)])

    def local_apply(u, a, bm, cm, diag):
        batch, nx, ny, nz = u.shape
        r, c = lax.axis_index("row"), lax.axis_index("col")
        peers = jnp.bitwise_xor(r, jnp.arange(4))
        sides = jnp.bitwise_xor(c, jnp.arange(2))
        slab = nx // 4
        a4 = jnp.take(a.reshape(4, slab, nx), peers, axis=0)
        a6 = a4.reshape(nx, nx).T
        b4 = jnp.take(bm.reshape(2, nx // 2, 4, nx // 4), sides, axis=0)
        b4 = jnp.take(b4, peers, axis=2).reshape(nx, nx)
        b5 = b4.T
        c_out = jnp.take(cm.reshape(nx, 2, nx // 2), sides, axis=1).reshape(nx, nx)
        c_in = c_out.T
        token = jnp.zeros((8, 128), F32)
        cuts = SLABS
        starts = [[sum(cut[:q]) for q in range(len(cut))] for cut in cuts]
        y_in, z_in, j_in, x_in = {}, {}, {}, {}
        w = None
        for kind, b, q in ORDER:
            if kind == 1:
                parts = [(starts[b][p], cuts[b][p]) for p in q]
                outs, token = stage_one(token, u, a4, b, parts, ny, nz)
                for m, part in enumerate(q):
                    y_in[b, part] = over_row(outs[4 * m:4 * m + 4], 3 * m)
            elif kind == 2:
                (own, other), token = stage_two(token, y_in.pop((b, q)), b4)
                z_in[b, q] = (own, over_col(other))
            elif kind == 3:
                own, got = z_in.pop((b, q))
                (own, other), token = stage_three_four(token, own, got, c_in, c_out, diag, starts[b][q])
                j_in[b, q] = (own, over_col(other))
            elif kind == 5:
                own, got = j_in.pop((b, q))
                outs, token = stage_five(token, own, got, b5)
                x_in[b, q] = over_row(outs)
            else:
                pieces = [x_in[b, p][k] for k in range(4) for p in range(len(cuts[b]))]
                w, token = stage_six(token, pieces, a6, w, b, batch)
        return w

    return jax.shard_map(local_apply, mesh=mesh, in_specs=(spec_field, spec_factor, spec_factor, spec_factor, spec_diag), out_specs=spec_field, check_vma=False)
```

```python
import jax
import jax.numpy as jnp
from jax import lax
from jax.experimental import pallas as pl
from jax.experimental.pallas import tpu as pltpu
from jax.sharding import PartitionSpec as P


BF = jnp.bfloat16
F32 = jnp.float32

SLABS = (
    (8, 16, 16, 24,),
    (32, 32,),
    (64,),
    (64,),
    (64,),
    (64,),
    (64,),
    (64,),
    (64,),
    (64,),
    (32, 32,),
    (16, 16, 16, 8, 8,),
)


ORDER = (
    (1, 0, (0, 1, 2, 3)), (0, 0, 0), (2, 0, 0), (2, 0, 1), (3, 0, 0), (2, 0, 2), (3, 0, 1), (1, 1, (0, 1)),
    (2, 0, 3), (3, 0, 2), (2, 1, 0), (5, 0, 1), (3, 0, 3), (5, 0, 2), (1, 2, (0,)), (5, 0, 0), (2, 1, 1),
    (3, 1, 0), (5, 0, 3), (2, 2, 0), (1, 3, (0,)), (3, 1, 1), (1, 4, (0,)), (5, 1, 0), (6, 0, 0),
    (1, 5, (0,)), (2, 3, 0), (3, 2, 0), (5, 1, 1), (3, 3, 0), (5, 2, 0), (2, 4, 0), (5, 3, 0), (6, 1, 0),
    (1, 6, (0,)), (2, 5, 0), (3, 4, 0), (6, 2, 0), (3, 5, 0), (1, 7, (0,)), (6, 3, 0), (5, 4, 0), (2, 6, 0),
    (5, 5, 0), (1, 8, (0,)), (2, 7, 0), (3, 6, 0), (1, 9, (0,)), (6, 4, 0), (2, 8, 0), (3, 7, 0), (5, 6, 0),
    (1, 10, (0, 1)), (2, 9, 0), (6, 6, 0), (3, 8, 0), (5, 7, 0), (2, 10, 0), (3, 9, 0), (5, 8, 0), (6, 5, 0),
    (6, 7, 0), (1, 11, (0, 1, 2, 3, 4)), (3, 10, 0), (2, 10, 1), (2, 11, 1), (5, 9, 0), (6, 8, 0), (2, 11, 0),
    (3, 10, 1), (5, 10, 0), (6, 9, 0), (3, 11, 0), (5, 10, 1), (2, 11, 2), (3, 11, 1), (5, 11, 0), (2, 11, 3),
    (3, 11, 2), (6, 10, 0), (5, 11, 1), (2, 11, 4), (3, 11, 3), (5, 11, 2), (3, 11, 4), (5, 11, 3),
    (5, 11, 4), (6, 11, 0),
)


def dot(a, b):
    return jnp.dot(a, b, preferred_element_type=F32)


def any_spec():
    return pl.BlockSpec(memory_space=pl.ANY)


def whole(shape):
    return pl.BlockSpec(shape, lambda *g: (0,) * len(shape))


TOKEN = jax.ShapeDtypeStruct((8, 128), F32)


def call(body, token, ins, in_specs, outs, out_specs, grid, flops, alias=None, scratch=()):
    n_in, n_out, lead = len(ins), len(outs), 0 if token is None else 1

    def wrapped(*refs):
        refs = refs[lead:]
        body(refs[:n_in], refs[n_in:n_in + n_out], *refs[n_in + n_out + 1:])

    aliases = {i + lead: o for i, o in (alias or {}).items()}
    if lead:
        aliases[0] = n_out
    results = pl.pallas_call(
        wrapped,
        grid=grid,
        in_specs=[any_spec()] * lead + list(in_specs),
        out_specs=list(out_specs) + [any_spec()],
        out_shape=list(outs) + [TOKEN],
        input_output_aliases=aliases,
        scratch_shapes=list(scratch),
        cost_estimate=pl.CostEstimate(flops=flops, bytes_accessed=1 << 20, transcendentals=0),
        compiler_params=pltpu.CompilerParams(vmem_limit_bytes=67043328),
    )(*([token] * lead), *ins)
    return results[:-1], results[-1]


def peer_rows(ref, me, k, size, offset=0, count=None):
    at = pl.multiple_of((me ^ k) * size, size) + offset
    return ref[pl.ds(at, count or size), :]


def prepare(token, a, bm, cm):
    n = a.shape[0]

    def body(ins, outs, rows):
        a_ref, b_ref, c_ref = ins
        a6, b4, b5, c_in, c_out = outs
        r, c = lax.axis_index("row"), lax.axis_index("col")
        a6[...] = jnp.concatenate([peer_rows(a_ref, r, k, n // 4) for k in range(4)], axis=0).T
        rows[...] = jnp.concatenate([peer_rows(b_ref, c, l, n // 2) for l in range(2)], axis=0).T
        back = jnp.concatenate([peer_rows(rows, r, k, n // 4) for k in range(4)], axis=0)
        b5[...] = back
        b4[...] = back.T
        half = n // 2
        out = jnp.concatenate([c_ref[:, pl.ds(pl.multiple_of((c ^ l) * half, half), half)] for l in range(2)], axis=1)
        c_out[...] = out
        c_in[...] = out.T

    spec = whole((n, n))
    return call(body, token, (a, bm, cm), [spec] * 3, [jax.ShapeDtypeStruct((n, n), BF)] * 5, [spec] * 5, (1,),
                1 << 20, scratch=[pltpu.VMEM((n, n), BF)])


def stage_one(token, u, a, b, parts, ny, nz, yb=16, sub=8):
    nx = u.shape[1]
    rows = 4 * sum(s for _, s in parts)

    def body(ins, outs):
        u_ref, a_ref = ins
        r = lax.axis_index("row")
        mine = jnp.concatenate([peer_rows(a_ref, r, k, nx // 4, o, s) for o, s in parts for k in range(4)], axis=0)

        def step(t, carry):
            at_y = pl.ds(pl.multiple_of(t * sub, sub), sub)
            flat = u_ref[0, :, at_y, :].reshape(nx, sub * nz)
            h = dot(mine, flat).astype(BF).reshape(rows, sub, nz)
            at = 0
            for n, (o, s) in enumerate(parts):
                for k in range(4):
                    outs[4 * n + k][:, at_y, :] = h[at:at + s]
                    at += s
            return carry

        lax.fori_loop(0, yb // sub, step, 0)

    outs = [jax.ShapeDtypeStruct((s, ny, nz), BF) for _, s in parts for _ in range(4)]
    out_specs = [pl.BlockSpec((s, yb, nz), lambda g: (0, g, 0)) for _, s in parts for _ in range(4)]
    return call(body, token, (u, a), [pl.BlockSpec((1, nx, yb, nz), lambda g: (b, 0, g, 0)), whole(a.shape)],
                outs, out_specs, (ny // yb,), 2 * rows * nx * ny * nz)


def block_of(size):
    return 16 if size % 16 == 0 else 8


def stage_two(token, pieces, b4):
    size, ny, nz = pieces[0].shape
    ti = block_of(size)
    nj = b4.shape[0] // 2

    def body(ins, outs):
        bm = ins[4][...]

        def step(t, carry):
            i = 2 * t
            y = jnp.concatenate([jnp.concatenate([ins[k][i + e] for k in range(4)], axis=0) for e in range(2)], axis=1)
            h = dot(bm, y).astype(BF)
            for e in range(2):
                for l in range(2):
                    outs[l][i + e] = h[l * nj:(l + 1) * nj, e * nz:(e + 1) * nz]
            return carry

        lax.fori_loop(0, ti // 2, step, 0, unroll=4 if size <= 8 else 2)

    out = jax.ShapeDtypeStruct((size, nj, nz), BF)
    return call(body, token, (*pieces, b4), [pl.BlockSpec((ti, ny, nz), lambda g: (g, 0, 0))] * 4 + [whole(b4.shape)],
                [out] * 2, [pl.BlockSpec((ti, nj, nz), lambda g: (g, 0, 0))] * 2, (size // ti,),
                2 * size * 4 * ny * 2 * nj * nz)


def stage_three_four(token, own, got, c_in, c_out, diag, offset):
    size, nj, nz = own.shape
    ti = block_of(size if offset % 16 == 0 else 8)
    nk = c_out.shape[0]

    def body(ins, outs):
        own_ref, got_ref, ci_ref, co_ref, d_ref = ins
        ci, co = ci_ref[...], co_ref[...]

        def step(t, carry):
            i = 2 * t
            z = jnp.concatenate([jnp.concatenate([own_ref[i + e], got_ref[i + e]], axis=1) for e in range(2)], axis=0)
            h3 = (dot(z, ci) * d_ref[pl.ds(i, 2)].reshape(2 * nj, nk)).astype(BF)
            h4 = dot(h3, co).astype(BF)
            for e in range(2):
                for l in range(2):
                    outs[l][i + e] = h4[e * nj:(e + 1) * nj, l * nz:(l + 1) * nz]
            return carry

        lax.fori_loop(0, ti // 2, step, 0, unroll=4 if size <= 8 else 2)

    first = offset // ti
    block = pl.BlockSpec((ti, nj, nz), lambda g: (g, 0, 0))
    out = jax.ShapeDtypeStruct((size, nj, nz), BF)
    return call(body, token, (own, got, c_in, c_out, diag),
                [block] * 2 + [whole(c_in.shape), whole(c_out.shape), pl.BlockSpec((ti, nj, nk), lambda g: (first + g, 0, 0))],
                [out] * 2, [block] * 2, (size // ti,), 4 * size * nj * 2 * nz * nk)


def stage_five(token, own, got, b5):
    size, nj, nz = own.shape
    ti = block_of(size)
    ny = b5.shape[0] // 4

    def body(ins, outs):
        bm = ins[2][...]

        def step(t, carry):
            i = 2 * t
            j = jnp.concatenate([jnp.concatenate([ins[l][i + e] for l in range(2)], axis=0) for e in range(2)], axis=1)
            h = dot(bm, j).astype(BF)
            for e in range(2):
                for k in range(4):
                    outs[k][i + e] = h[k * ny:(k + 1) * ny, e * nz:(e + 1) * nz]
            return carry

        lax.fori_loop(0, ti // 2, step, 0, unroll=4 if size <= 8 else 2)

    out = jax.ShapeDtypeStruct((size, ny, nz), BF)
    return call(body, token, (own, got, b5), [pl.BlockSpec((ti, nj, nz), lambda g: (g, 0, 0))] * 2 + [whole(b5.shape)],
                [out] * 4, [pl.BlockSpec((ti, ny, nz), lambda g: (g, 0, 0))] * 4, (size // ti,),
                2 * size * 2 * nj * 4 * ny * nz)


def stage_six(token, pieces, a6, w, b, batch, yb=16, sub=8):
    nx = a6.shape[0]
    _, ny, nz = pieces[0].shape
    n = len(pieces)

    def body(ins, outs):
        def step(t, carry):
            at_y = pl.ds(pl.multiple_of(t * sub, sub), sub)
            x = jnp.concatenate([ref[:, at_y, :] for ref in ins[:n]], axis=0).reshape(a6.shape[1], sub * nz)
            outs[0][0, :, at_y, :] = dot(ins[n][...], x).reshape(nx, sub, nz)
            return carry

        lax.fori_loop(0, yb // sub, step, 0)

    ins = (*pieces, a6)
    in_specs = [pl.BlockSpec((p.shape[0], yb, nz), lambda g: (0, g, 0)) for p in pieces] + [whole(a6.shape)]
    alias = None
    if w is not None:
        ins += (w,)
        in_specs.append(any_spec())
        alias = {len(ins) - 1: 0}
    (w,), token = call(body, token, ins, in_specs, [jax.ShapeDtypeStruct((batch, nx, ny, nz), F32)],
                       [pl.BlockSpec((1, nx, yb, nz), lambda g: (b, 0, g, 0))], (ny // yb,),
                       2 * nx * nx * ny * nz, alias)
    return w, token


def solution(mesh):
    spec_field = P("fields", None, "row", "col")
    spec_factor = P("fields", None)
    spec_diag = P(("fields", "row"), "col", None)

    def over_row(outs, m=0):
        got = {}
        for k in (2, 3, 1):
            got[k] = lax.ppermute(outs[k], "row", [(r, r ^ k) for r in range(4)])
            m += 1
        return [outs[0], got[1], got[2], got[3]]

    def over_col(value):
        return lax.ppermute(value, "col", [(0, 1), (1, 0)])

    def local_apply(u, a, bm, cm, diag):
        batch, _, ny, nz = u.shape
        token = None
        cuts = SLABS
        starts = [[sum(cut[:q]) for q in range(len(cut))] for cut in cuts]
        y_in, z_in, j_in, x_in = {}, {}, {}, {}
        w = None
        for kind, b, q in ORDER:
            if kind == 1:
                parts = [(starts[b][p], cuts[b][p]) for p in q]
                outs, token = stage_one(token, u, a, b, parts, ny, nz)
                for m, part in enumerate(q):
                    y_in[b, part] = over_row(outs[4 * m:4 * m + 4], 3 * m)
            elif kind == 0:
                (a6, b4, b5, c_in, c_out), token = prepare(token, a, bm, cm)
            elif kind == 2:
                (own, other), token = stage_two(token, y_in.pop((b, q)), b4)
                z_in[b, q] = (own, over_col(other))
            elif kind == 3:
                own, got = z_in.pop((b, q))
                (own, other), token = stage_three_four(token, own, got, c_in, c_out, diag, starts[b][q])
                j_in[b, q] = (own, over_col(other))
            elif kind == 5:
                own, got = j_in.pop((b, q))
                outs, token = stage_five(token, own, got, b5)
                x_in[b, q] = over_row(outs)
            else:
                pieces = [x_in[b, p][k] for k in range(4) for p in range(len(cuts[b]))]
                w, token = stage_six(token, pieces, a6, w, b, batch)
        return w

    return jax.shard_map(local_apply, mesh=mesh, in_specs=(spec_field, spec_factor, spec_factor, spec_factor, spec_diag), out_specs=spec_field, check_vma=False)
```

```python
import jax
import jax.numpy as jnp
from jax import lax
from jax.experimental import pallas as pl
from jax.experimental.pallas import tpu as pltpu
from jax.sharding import PartitionSpec as P


BF = jnp.bfloat16
F32 = jnp.float32

SLABS = ((8, 16, 16, 24,), (32, 32,)) + ((64,),) * 8 + ((32, 32,), (16, 16, 16, 8, 8,))


ORDER = (
    1000, 0, 2000, 2001, 3000, 2002, 3001, 1010, 2003, 3002, 2010, 5001, 3003, 5002, 1020, 5000, 2011, 3010,
    5003, 2020, 1030, 3011, 1040, 5010, 6000, 1050, 2030, 3020, 5011, 3030, 5020, 2040, 5030, 6010, 1060,
    2050, 3040, 6020, 3050, 1070, 6030, 5040, 2060, 5050, 1080, 2070, 3060, 1090, 6040, 2080, 3070, 5060,
    1100, 2090, 6060, 3080, 5070, 2100, 3090, 5080, 6050, 6070, 1110, 3100, 2101, 2111, 5090, 6080, 2110,
    3101, 5100, 6090, 3110, 5101, 2112, 3111, 5110, 2113, 3112, 6100, 5111, 2114, 3113, 5112, 3114, 5113,
    5114, 6110,
)


def decode(code):
    kind, rest = divmod(code, 1000)
    return kind, *divmod(rest, 10)


def dot(a, b):
    return jnp.dot(a, b, preferred_element_type=F32)


def any_spec():
    return pl.BlockSpec(memory_space=pl.ANY)


def whole(shape):
    return pl.BlockSpec(shape, lambda *g: (0,) * len(shape))


TOKEN = jax.ShapeDtypeStruct((8, 128), F32)


def call(body, token, ins, in_specs, outs, out_specs, grid, flops, alias=None, scratch=()):
    n_in, n_out, lead = len(ins), len(outs), 0 if token is None else 1

    def wrapped(*refs):
        refs = refs[lead:]
        body(refs[:n_in], refs[n_in:n_in + n_out], *refs[n_in + n_out + 1:])

    aliases = {i + lead: o for i, o in (alias or {}).items()}
    if lead:
        aliases[0] = n_out
    results = pl.pallas_call(
        wrapped,
        grid=grid,
        in_specs=[any_spec()] * lead + list(in_specs),
        out_specs=list(out_specs) + [any_spec()],
        out_shape=list(outs) + [TOKEN],
        input_output_aliases=aliases,
        scratch_shapes=list(scratch),
        cost_estimate=pl.CostEstimate(flops=flops, bytes_accessed=1 << 20, transcendentals=0),
        compiler_params=pltpu.CompilerParams(vmem_limit_bytes=67043328),
    )(*([token] * lead), *ins)
    return results[:-1], results[-1]


def peer_rows(ref, me, k, size, offset=0, count=None):
    at = pl.multiple_of((me ^ k) * size, size) + offset
    return ref[pl.ds(at, count or size), :]


def prepare(token, a, bm, cm):
    n = a.shape[0]

    def body(ins, outs, rows):
        a_ref, b_ref, c_ref = ins
        a6, b4, b5, c_in, c_out = outs
        r, c = lax.axis_index("row"), lax.axis_index("col")
        a6[...] = jnp.concatenate([peer_rows(a_ref, r, k, n // 4) for k in range(4)], axis=0).T
        rows[...] = jnp.concatenate([peer_rows(b_ref, c, l, n // 2) for l in range(2)], axis=0).T
        back = jnp.concatenate([peer_rows(rows, r, k, n // 4) for k in range(4)], axis=0)
        b5[...] = back
        b4[...] = back.T
        half = n // 2
        out = jnp.concatenate([c_ref[:, pl.ds(pl.multiple_of((c ^ l) * half, half), half)] for l in range(2)], axis=1)
        c_out[...] = out
        c_in[...] = out.T

    spec = whole((n, n))
    return call(body, token, (a, bm, cm), [spec] * 3, [jax.ShapeDtypeStruct((n, n), BF)] * 5, [spec] * 5, (1,),
                1 << 20, scratch=[pltpu.VMEM((n, n), BF)])


def stage_one(token, u, a, b, parts, ny, nz, yb=16, sub=8):
    nx = u.shape[1]
    rows = 4 * sum(s for _, s in parts)

    def body(ins, outs):
        u_ref, a_ref = ins
        r = lax.axis_index("row")
        mine = jnp.concatenate([peer_rows(a_ref, r, k, nx // 4, o, s) for o, s in parts for k in range(4)], axis=0)

        def step(t, carry):
            at_y = pl.ds(pl.multiple_of(t * sub, sub), sub)
            flat = u_ref[0, :, at_y, :].reshape(nx, sub * nz)
            h = dot(mine, flat).astype(BF).reshape(rows, sub, nz)
            at = 0
            for n, (o, s) in enumerate(parts):
                for k in range(4):
                    outs[4 * n + k][:, at_y, :] = h[at:at + s]
                    at += s
            return carry

        lax.fori_loop(0, yb // sub, step, 0)

    outs = [jax.ShapeDtypeStruct((s, ny, nz), BF) for _, s in parts for _ in range(4)]
    out_specs = [pl.BlockSpec((s, yb, nz), lambda g: (0, g, 0)) for _, s in parts for _ in range(4)]
    return call(body, token, (u, a), [pl.BlockSpec((1, nx, yb, nz), lambda g: (b, 0, g, 0)), whole(a.shape)],
                outs, out_specs, (ny // yb,), 2 * rows * nx * ny * nz)


def block_of(size):
    return 16 if size % 16 == 0 else 8


def stage_two(token, pieces, b4):
    size, ny, nz = pieces[0].shape
    ti = block_of(size)
    nj = b4.shape[0] // 2

    def body(ins, outs):
        bm = ins[4][...]

        def step(t, carry):
            i = 2 * t
            y = jnp.concatenate([jnp.concatenate([ins[k][i + e] for k in range(4)], axis=0) for e in range(2)], axis=1)
            h = dot(bm, y).astype(BF)
            for e in range(2):
                for l in range(2):
                    outs[l][i + e] = h[l * nj:(l + 1) * nj, e * nz:(e + 1) * nz]
            return carry

        lax.fori_loop(0, ti // 2, step, 0, unroll=4 if size <= 8 else 2)

    out = jax.ShapeDtypeStruct((size, nj, nz), BF)
    return call(body, token, (*pieces, b4), [pl.BlockSpec((ti, ny, nz), lambda g: (g, 0, 0))] * 4 + [whole(b4.shape)],
                [out] * 2, [pl.BlockSpec((ti, nj, nz), lambda g: (g, 0, 0))] * 2, (size // ti,),
                2 * size * 4 * ny * 2 * nj * nz)


def stage_three_four(token, own, got, c_in, c_out, diag, offset):
    size, nj, nz = own.shape
    ti = block_of(size if offset % 16 == 0 else 8)
    nk = c_out.shape[0]

    def body(ins, outs):
        own_ref, got_ref, ci_ref, co_ref, d_ref = ins
        ci, co = ci_ref[...], co_ref[...]

        def step(t, carry):
            i = 2 * t
            z = jnp.concatenate([jnp.concatenate([own_ref[i + e], got_ref[i + e]], axis=1) for e in range(2)], axis=0)
            h3 = (dot(z, ci) * d_ref[pl.ds(i, 2)].reshape(2 * nj, nk)).astype(BF)
            h4 = dot(h3, co).astype(BF)
            for e in range(2):
                for l in range(2):
                    outs[l][i + e] = h4[e * nj:(e + 1) * nj, l * nz:(l + 1) * nz]
            return carry

        lax.fori_loop(0, ti // 2, step, 0, unroll=4 if size <= 8 else 2)

    first = offset // ti
    block = pl.BlockSpec((ti, nj, nz), lambda g: (g, 0, 0))
    out = jax.ShapeDtypeStruct((size, nj, nz), BF)
    return call(body, token, (own, got, c_in, c_out, diag),
                [block] * 2 + [whole(c_in.shape), whole(c_out.shape), pl.BlockSpec((ti, nj, nk), lambda g: (first + g, 0, 0))],
                [out] * 2, [block] * 2, (size // ti,), 4 * size * nj * 2 * nz * nk)


def stage_five(token, own, got, b5):
    size, nj, nz = own.shape
    ti = block_of(size)
    ny = b5.shape[0] // 4

    def body(ins, outs):
        bm = ins[2][...]

        def step(t, carry):
            i = 2 * t
            j = jnp.concatenate([jnp.concatenate([ins[l][i + e] for l in range(2)], axis=0) for e in range(2)], axis=1)
            h = dot(bm, j).astype(BF)
            for e in range(2):
                for k in range(4):
                    outs[k][i + e] = h[k * ny:(k + 1) * ny, e * nz:(e + 1) * nz]
            return carry

        lax.fori_loop(0, ti // 2, step, 0, unroll=4 if size <= 8 else 2)

    out = jax.ShapeDtypeStruct((size, ny, nz), BF)
    return call(body, token, (own, got, b5), [pl.BlockSpec((ti, nj, nz), lambda g: (g, 0, 0))] * 2 + [whole(b5.shape)],
                [out] * 4, [pl.BlockSpec((ti, ny, nz), lambda g: (g, 0, 0))] * 4, (size // ti,),
                2 * size * 2 * nj * 4 * ny * nz)


def stage_six(token, pieces, a6, w, b, batch, yb=16, sub=8):
    nx = a6.shape[0]
    _, ny, nz = pieces[0].shape
    n = len(pieces)

    def body(ins, outs):
        def step(t, carry):
            at_y = pl.ds(pl.multiple_of(t * sub, sub), sub)
            x = jnp.concatenate([ref[:, at_y, :] for ref in ins[:n]], axis=0).reshape(a6.shape[1], sub * nz)
            outs[0][0, :, at_y, :] = dot(ins[n][...], x).reshape(nx, sub, nz)
            return carry

        lax.fori_loop(0, yb // sub, step, 0)

    ins = (*pieces, a6)
    in_specs = [pl.BlockSpec((p.shape[0], yb, nz), lambda g: (0, g, 0)) for p in pieces] + [whole(a6.shape)]
    alias = None
    if w is not None:
        ins += (w,)
        in_specs.append(any_spec())
        alias = {len(ins) - 1: 0}
    (w,), token = call(body, token, ins, in_specs, [jax.ShapeDtypeStruct((batch, nx, ny, nz), F32)],
                       [pl.BlockSpec((1, nx, yb, nz), lambda g: (b, 0, g, 0))], (ny // yb,),
                       2 * nx * nx * ny * nz, alias)
    return w, token


def solution(mesh):
    spec_field = P("fields", None, "row", "col")
    spec_factor = P("fields", None)
    spec_diag = P(("fields", "row"), "col", None)

    def over_row(outs, m=0):
        got = {}
        for k in (2, 3, 1):
            got[k] = lax.ppermute(outs[k], "row", [(r, r ^ k) for r in range(4)])
            m += 1
        return [outs[0], got[1], got[2], got[3]]

    def over_col(value):
        return lax.ppermute(value, "col", [(0, 1), (1, 0)])

    def local_apply(u, a, bm, cm, diag):
        batch, _, ny, nz = u.shape
        token = None
        cuts = SLABS
        starts = [[sum(cut[:q]) for q in range(len(cut))] for cut in cuts]
        y_in, z_in, j_in, x_in = {}, {}, {}, {}
        w = None
        for code in ORDER:
            kind, b, q = decode(code)
            if kind == 1:
                parts = list(zip(starts[b], cuts[b]))
                outs, token = stage_one(token, u, a, b, parts, ny, nz)
                for m in range(len(parts)):
                    y_in[b, m] = over_row(outs[4 * m:4 * m + 4], 3 * m)
            elif kind == 0:
                (a6, b4, b5, c_in, c_out), token = prepare(token, a, bm, cm)
            elif kind == 2:
                (own, other), token = stage_two(token, y_in.pop((b, q)), b4)
                z_in[b, q] = (own, over_col(other))
            elif kind == 3:
                own, got = z_in.pop((b, q))
                (own, other), token = stage_three_four(token, own, got, c_in, c_out, diag, starts[b][q])
                j_in[b, q] = (own, over_col(other))
            elif kind == 5:
                own, got = j_in.pop((b, q))
                outs, token = stage_five(token, own, got, b5)
                x_in[b, q] = over_row(outs)
            else:
                pieces = [x_in[b, p][k] for k in range(4) for p in range(len(cuts[b]))]
                w, token = stage_six(token, pieces, a6, w, b, batch)
        return w

    return jax.shard_map(local_apply, mesh=mesh, in_specs=(spec_field, spec_factor, spec_factor, spec_factor, spec_diag), out_specs=spec_field, check_vma=False)
```
